32 devices in a mesh: expert: 8 (over z, x), dp: 4 (over y, core).
Axes of the slice: x: 2, y: 2, z: 4, core: 2. Of those that a mesh axis runs over, the one named last changes fastest.
Arguments:
- tokens: bfloat16 [8192, 5120], P(('dp', 'expert')), parts along dimension 0, may hold values from -6 to 6
- router_logit: float32 [8192], P(('dp', 'expert')), parts along dimension 0, may hold values from 0 to 3
- expert_id: int32 [8192], P(('dp', 'expert')), parts along dimension 0, may hold values from 0 to 7, as said below
- token_slot: int32 [8192], P(('dp', 'expert')), parts along dimension 0, may hold values from 0 to 63, as said below
- keep: int32 [8192], P(('dp', 'expert')), parts along dimension 0, may hold values 0 or 1
- overflow_host: int32 [8, 32], replicated, may hold values from 0 to 7, as said below
- expert_gate: bfloat16 [8, 5120, 256], P('expert'), may hold values from -0.125 to 0.125
- expert_up: bfloat16 [8, 5120, 256], P('expert'), may hold values from -0.125 to 0.125
- expert_down: bfloat16 [8, 256, 5120], P('expert'), may hold values from -0.375 to 0.375
- shared_gate: bfloat16 [5120, 64], replicated, may hold values from -0.078125 to 0.078125
- shared_up: bfloat16 [5120, 64], replicated, may hold values from -0.078125 to 0.078125
- shared_down: bfloat16 [64, 5120], replicated, may hold values from -0.1875 to 0.1875
Outputs:
- moe_out: bfloat16 [8192, 5120], P(('dp', 'expert')), parts along dimension 0
The draws below stay inside these ranges and needn't reach their ends.
There are 4 independent parts, one for each index of `dp`. The reference program is written for one: setup_inputs(seed, part) draws one part's arguments, and reference() takes and returns one part's arrays. A program takes and returns all parts, laid end to end along the dimension named above; an argument that names none is the same for every part. Nothing has to cross between parts.
Inputs may be any that keep to these rules, and one draw needn't show every extreme that they name: `expert_id`: among the 256 tokens of one device at most 64 name the same expert; some experts are named by exactly 64 tokens of every device. `token_slot`: if c tokens of one device name the same expert, their slots are 0 to c - 1, each once. overflow_host[e, j] is e + 1 or e - 1, taken modulo 8.
All inputs are finite; a program needn't handle non-finite values. No bound on the sum of `keep` on one device may be relied on, other than what follows from the above.
Results may differ from the reference program's by a relative error of at most 0.007.
Values may be sent and summed in bfloat16 or wider, within the bound.
A program may use at most 128 MiB of HBM per device.

```python
import jax
import jax.numpy as jnp
from jax import lax

D = 5120
F = 256
SH = 64
T_DEV = 256
EXPERTS = 8
TOKENS = 2048
SLOTS = 64
HOME = 32
SPILL = 32


def draw_tokens(key, part):
    base_key = jax.random.fold_in(key, 31)
    key_row, key_value = jax.random.split(base_key, 2)
    values = jnp.clip(jax.random.normal(key_value, (TOKENS, D), jnp.float32), -6.0, 6.0)
    return values.astype(jnp.bfloat16)


def routing_pair(key):
    base_key = jax.random.fold_in(key, 11)
    key_hot, key_score, key_order = jax.random.split(base_key, 3)
    devices = TOKENS // T_DEV
    cell_count = EXPERTS * SLOTS
    hot_count = max(1, EXPERTS // 8)
    hot_rank = jax.random.permutation(key_hot, EXPERTS)
    is_hot = (hot_rank < hot_count).astype(jnp.int32)
    cell_ids = jnp.arange(cell_count, dtype=jnp.int32)
    noise_bits = jax.random.randint(key_score, (devices, cell_count), 0, 1 << 16)
    cell_score = is_hot[cell_ids // SLOTS][None, :] * (1 << 28) + noise_bits * cell_count + cell_ids[None, :]
    unused, chosen = lax.top_k(cell_score, T_DEV)
    device_ids = jnp.arange(devices, dtype=jnp.int32)[:, None]
    picked = jnp.zeros((devices, cell_count), jnp.int32).at[device_ids, chosen].set(1)
    slot_rank = jnp.cumsum(picked.reshape(devices, EXPERTS, SLOTS), axis=2).reshape(devices, cell_count) - 1
    chosen_rank = jnp.take_along_axis(slot_rank, chosen, axis=1)
    order_keys = jax.random.randint(key_order, (devices, T_DEV), 0, 1 << 16) * T_DEV + jnp.arange(T_DEV, dtype=jnp.int32)[None, :]
    token_order = jnp.argsort(order_keys, axis=1)
    token_cell = jnp.take_along_axis(chosen, token_order, axis=1)
    token_slots = jnp.take_along_axis(chosen_rank, token_order, axis=1)
    return ((token_cell // SLOTS).reshape(-1).astype(jnp.int32), token_slots.reshape(-1).astype(jnp.int32))


def draw_expert_id(key, part):
    return routing_pair(key)[0]


def draw_token_slot(key, part):
    return routing_pair(key)[1]


def draw_overflow_host(key, part):
    side_bits = jax.random.randint(jax.random.fold_in(key, 23), (EXPERTS, SPILL), 0, 2)
    expert_ids = jnp.arange(EXPERTS, dtype=jnp.int32)[:, None]
    return ((expert_ids + 2 * side_bits - 1 + EXPERTS) % EXPERTS).astype(jnp.int32)


def with_ends(values, stream_key, least, largest):
    longest = values.shape.index(max(values.shape))
    spots = []
    for shift in (0, 1):
        where = [jax.random.randint(jax.random.fold_in(stream_key, axis), (), 0, length) for axis, length in enumerate(values.shape)]
        where[longest] = (where[longest] + shift) % values.shape[longest]
        spots.append(tuple(where))
    return values.at[spots[0]].set(least).at[spots[1]].set(largest)


def level_of(own_key, dims, shards, least, top_value):
    gain, own = 1.0, jax.random.fold_in(own_key, 6)
    for dim, parts in shards:
        draws = jnp.exp(jax.random.uniform(jax.random.fold_in(own, dim), (parts,), jnp.float32, least / len(shards), top_value / len(shards)))
        gain = gain * jnp.repeat(draws, dims[dim] // parts).reshape([-1 if axis == dim else 1 for axis in range(len(dims))])
    return gain


def normal_values(own_key, shape, width, reach, shards=(), kind=jnp.bfloat16):
    gain = level_of(own_key, shape, shards, -0.22, 0.18) if shards else 1.0
    entries = jax.random.normal(own_key, shape, jnp.float32) * width * gain
    return jnp.minimum(jnp.maximum(entries, -reach), reach).astype(kind)


def setup_inputs(seed: int = 0, part: int = 0) -> dict:
    key_list = jax.random.split(jax.random.key(seed), 13)
    part_splits = jax.random.split(jax.random.fold_in(key_list[12], part), 13)
    return {
        "tokens": draw_tokens(jax.random.fold_in(jax.random.fold_in(key_list[12], part), 71), part),
        "router_logit": jnp.clip(3.0 * jax.random.uniform(part_splits[1], (TOKENS,), jnp.float32) ** level_of(part_splits[1], (TOKENS,), ((0, 8),), -0.2, 0.2), 0.0, 3.0),
        "expert_id": draw_expert_id(jax.random.fold_in(jax.random.fold_in(key_list[12], part), 71), part),
        "token_slot": draw_token_slot(jax.random.fold_in(jax.random.fold_in(key_list[12], part), 71), part),
        "keep": with_ends((jax.random.randint(part_splits[4], (TOKENS,), 0, 8) < 7).astype(jnp.int32), jax.random.fold_in(part_splits[4], 1), 0, 1),
        "overflow_host": draw_overflow_host(jax.random.fold_in(key_list[12], 71), part),
        "expert_gate": normal_values(key_list[6], (EXPERTS, D, F), (D // 2) ** -0.5, 0.125, ((0, 8),)),
        "expert_up": normal_values(key_list[7], (EXPERTS, D, F), (D // 2) ** -0.5, 0.125, ((0, 8),)),
        "expert_down": normal_values(key_list[8], (EXPERTS, F, D), F ** -0.5, 0.375, ((0, 8),)),
        "shared_gate": normal_values(key_list[9], (D, SH), D ** -0.5, 0.078125),
        "shared_up": normal_values(key_list[10], (D, SH), D ** -0.5, 0.078125),
        "shared_down": normal_values(key_list[11], (SH, D), (16 * SH) ** -0.5, 0.1875),
    }


def reference(tokens, router_logit, expert_id, token_slot, keep, overflow_host, expert_gate, expert_up, expert_down, shared_gate, shared_up, shared_down):
    token_scale = jax.nn.sigmoid(router_logit) * keep.astype(jnp.float32)
    routed_in = (tokens.astype(jnp.float32) * token_scale[:, None]).astype(jnp.bfloat16)
    is_spill = token_slot >= HOME
    spill_level = jnp.maximum(token_slot - HOME, 0).astype(jnp.int32)
    host_expert = overflow_host[expert_id, spill_level].astype(jnp.int32)
    served = jnp.where(is_spill, host_expert, expert_id).astype(jnp.int32)
    lane_count = HOME + 2 * SPILL
    positions = jnp.arange(TOKENS, dtype=jnp.int32)
    source_device = positions // T_DEV
    to_right = host_expert == (expert_id + 1) % EXPERTS
    lane_index = jnp.where(is_spill, jnp.where(to_right, HOME + spill_level, HOME + SPILL + spill_level), token_slot)
    column_index = (source_device * lane_count + lane_index).astype(jnp.int32)
    token_table = jnp.full((EXPERTS, EXPERTS * lane_count), TOKENS, jnp.int32).at[served, column_index].set(positions)
    padded = jnp.concatenate([routed_in, jnp.zeros((1, D), jnp.bfloat16)], axis=0)

    def one_expert(partial_value, inputs):
        index_row, w_gate, w_up, w_down = inputs
        chosen = padded[index_row]
        gate_out = jnp.dot(chosen, w_gate, preferred_element_type=jnp.float32)
        up_out = jnp.dot(chosen, w_up, preferred_element_type=jnp.float32)
        hidden = (jax.nn.silu(gate_out) * up_out).astype(jnp.bfloat16)
        result = jnp.dot(hidden, w_down, preferred_element_type=jnp.float32).astype(jnp.bfloat16)
        return partial_value.at[index_row].set(result), None

    routed, unused = lax.scan(one_expert, jnp.zeros((TOKENS + 1, D), jnp.bfloat16), (token_table, expert_gate, expert_up, expert_down))
    shared_hidden = (jax.nn.silu(jnp.dot(tokens, shared_gate, preferred_element_type=jnp.float32)) * jnp.dot(tokens, shared_up, preferred_element_type=jnp.float32)).astype(jnp.bfloat16)
    shared_out = jnp.dot(shared_hidden, shared_down, preferred_element_type=jnp.float32)
    return (shared_out + routed[:TOKENS].astype(jnp.float32)).astype(jnp.bfloat16)
```

```python
import jax
import jax.numpy as jnp
from jax import lax
from jax.sharding import PartitionSpec as P


def expert_ffn(inputs, w_gate, w_up, w_down):
    flat_rows = inputs.reshape(-1, inputs.shape[-1])
    gate_out = jnp.dot(flat_rows, w_gate, preferred_element_type=jnp.float32)
    up_out = jnp.dot(flat_rows, w_up, preferred_element_type=jnp.float32)
    hidden = (jax.nn.silu(gate_out) * up_out).astype(jnp.bfloat16)
    result = jnp.dot(hidden, w_down, preferred_element_type=jnp.float32).astype(jnp.bfloat16)
    return result.reshape(inputs.shape)


def body(
    tokens,
    router_logit,
    expert_id,
    token_slot,
    keep,
    overflow_host,
    expert_gate,
    expert_up,
    expert_down,
    shared_gate,
    shared_up,
    shared_down,
):
    experts = lax.axis_size("expert")
    tok_count = tokens.shape[0]
    model_width = tokens.shape[1]
    slot_count = 2 * tok_count // experts
    home_count = slot_count // 2
    spill_count = slot_count - home_count
    w_gate = expert_gate[0]
    w_up = expert_up[0]
    w_down = expert_down[0]
    token_scale = jax.nn.sigmoid(router_logit) * keep.astype(jnp.float32)
    routed_in = (tokens.astype(jnp.float32) * token_scale[:, None]).astype(jnp.bfloat16)
    positions = jnp.arange(tok_count, dtype=jnp.int32)
    is_spill = token_slot >= home_count
    spill_level = jnp.maximum(token_slot - home_count, 0)
    table_index = expert_id * spill_count + spill_level
    table_ids = jnp.arange(experts * spill_count, dtype=jnp.int32)
    host_expert = jnp.sum(
        jnp.where(table_index[:, None] == table_ids[None, :], overflow_host.reshape(1, -1), 0),
        axis=1,
    )
    target = jnp.where(is_spill, host_expert, expert_id)
    spill_key = jnp.where(is_spill, host_expert, -1 - positions)
    earlier = (spill_key[:, None] == spill_key[None, :]) & (positions[None, :] < positions[:, None])
    spill_rank = jnp.sum(earlier.astype(jnp.int32), axis=1)
    need = jnp.max(jnp.where(is_spill, spill_rank + 1, 0))
    need = jnp.max(lax.all_gather(jnp.full((1, 128), need, jnp.int32), ("dp", "expert")))
    lane_index = jnp.where(is_spill, home_count + spill_rank, token_slot)

    def exchange(extra):
        lanes = home_count + extra

        def run(rows):
            cell_index = target * lanes + lane_index
            source_row = jnp.zeros((experts * lanes,), jnp.int32).at[cell_index].set(
                positions, mode="drop"
            )
            outgoing = rows[source_row].reshape(experts, lanes, model_width)
            incoming = lax.all_to_all(outgoing, "expert", split_axis=0, concat_axis=0, tiled=True)
            answers = lax.all_to_all(
                expert_ffn(incoming, w_gate, w_up, w_down),
                "expert",
                split_axis=0,
                concat_axis=0,
                tiled=True,
            )
            return answers.reshape(-1, model_width)[cell_index]

        return run

    most = 2 * spill_count
    levels = [max(1, most * part // 16) for part in (5, 6, 8, 16)]
    chosen = sum((need > level).astype(jnp.int32) for level in levels[:-1])
    routed = lax.switch(chosen, [exchange(level) for level in levels], routed_in)
    shared_hidden = (
        jax.nn.silu(jnp.dot(tokens, shared_gate, preferred_element_type=jnp.float32))
        * jnp.dot(tokens, shared_up, preferred_element_type=jnp.float32)
    ).astype(jnp.bfloat16)
    shared_out = jnp.dot(shared_hidden, shared_down, preferred_element_type=jnp.float32)
    return (shared_out + routed.astype(jnp.float32)).astype(jnp.bfloat16)


def solution(mesh):
    return jax.shard_map(
        body,
        mesh=mesh,
        in_specs=(
            P(("dp", "expert"), None),
            P(("dp", "expert")),
            P(("dp", "expert")),
            P(("dp", "expert")),
            P(("dp", "expert")),
            P(),
            P("expert", None, None),
            P("expert", None, None),
            P("expert", None, None),
            P(),
            P(),
            P(),
        ),
        out_specs=P(("dp", "expert"), None),
        check_vma=False,
    )
```

```python
import functools

import jax
import jax.numpy as jnp
from jax import lax
from jax.experimental import pallas as pl
from jax.experimental.pallas import tpu as pltpu
from jax.sharding import PartitionSpec as P

MESH = pl.DeviceIdType.MESH


def expert_ffn(inputs, w_gate, w_up, w_down):
    flat_rows = inputs.reshape(-1, inputs.shape[-1])
    gate_out = jnp.dot(flat_rows, w_gate, preferred_element_type=jnp.float32)
    up_out = jnp.dot(flat_rows, w_up, preferred_element_type=jnp.float32)
    hidden = (jax.nn.silu(gate_out) * up_out).astype(jnp.bfloat16)
    result = jnp.dot(hidden, w_down, preferred_element_type=jnp.float32).astype(jnp.bfloat16)
    return result.reshape(inputs.shape)


def meta_kernel(dps, experts, meta_ref, all_ref, own_sem, send_sem, recv_sem):
    my_dp, my_e = lax.axis_index("dp"), lax.axis_index("expert")
    total = dps * experts
    me = my_dp * experts + my_e
    own = pltpu.make_async_copy(meta_ref, all_ref.at[me], own_sem)
    own.start()

    def copy_to(k):
        there = lax.rem(me + k, total)
        return pltpu.make_async_remote_copy(
            src_ref=meta_ref,
            dst_ref=all_ref.at[me],
            send_sem=send_sem.at[k],
            recv_sem=recv_sem.at[k],
            device_id={"dp": there // experts, "expert": lax.rem(there, experts)},
            device_id_type=MESH,
        )

    @pl.loop(1, total)
    def _(k):
        copy_to(k).start()

    @pl.loop(1, total)
    def _(k):
        copy_to(k).wait_recv()

    @pl.loop(1, total)
    def _(k):
        copy_to(k).wait_send()

    own.wait()


def gather_meta(meta):
    dps, experts = lax.axis_size("dp"), lax.axis_size("expert")
    total = dps * experts
    return pl.pallas_call(
        functools.partial(meta_kernel, dps, experts),
        out_shape=jax.ShapeDtypeStruct((total,) + meta.shape, meta.dtype),
        in_specs=[pl.BlockSpec(memory_space=pltpu.VMEM)],
        out_specs=pl.BlockSpec(memory_space=pltpu.VMEM),
        scratch_shapes=[
            pltpu.SemaphoreType.DMA,
            pltpu.SemaphoreType.DMA((total,)),
            pltpu.SemaphoreType.DMA((total,)),
        ],
        compiler_params=pltpu.CompilerParams(has_side_effects=True),
        name="meta",
    )(meta)


def moe_kernel(
    experts,
    groups,
    home_out,
    spill_out,
    mask_ref,
    tok_ref,
    wg_hbm,
    wu_hbm,
    wd_hbm,
    sg_ref,
    su_ref,
    home_ret,
    spill_ret,
    shared_ref,
    home_in,
    home_res,
    spill_in,
    spill_res,
    spill_part,
    spill_comb,
    wg,
    wu,
    wd,
    w_sem,
    own_sem,
    hs_sem,
    hr_sem,
    rs_sem,
    rr_sem,
    zs_sem,
    zr_sem,
    xs_sem,
    xr_sem,
    ps_sem,
    pr_sem,
    cs_sem,
    cr_sem,
):
    e = lax.axis_index("expert")
    g = e // 2
    p = e - 2 * g
    partner = e + 1 - 2 * p

    weights = [
        pltpu.make_async_copy(a, b, w_sem.at[i])
        for i, (a, b) in enumerate(((wg_hbm, wg), (wu_hbm, wu), (wd_hbm, wd)))
    ]
    for copy in weights:
        copy.start()
    own = [
        pltpu.make_async_copy(home_out.at[e], home_in.at[e], own_sem.at[0]),
        pltpu.make_async_copy(spill_out.at[g], spill_in.at[0, g], own_sem.at[1]),
    ]
    for copy in own:
        copy.start()

    def remote(src, dst, send, recv, to):
        return pltpu.make_async_remote_copy(
            src_ref=src,
            dst_ref=dst,
            send_sem=send,
            recv_sem=recv,
            device_id={"expert": to},
            device_id_type=MESH,
        )

    def z_copy(k):
        to = lax.rem(g + k, groups)
        return remote(spill_out.at[to], spill_in.at[0, g], zs_sem.at[k], zr_sem.at[k], 2 * to + p)

    def h_copy(k):
        to = lax.rem(e + k, experts)
        return remote(home_out.at[to], home_in.at[e], hs_sem.at[k], hr_sem.at[k], to)

    def x_copy(k):
        origin = lax.rem(g - k + groups, groups)
        return remote(
            spill_in.at[0, origin], spill_in.at[1, origin], xs_sem.at[k], xr_sem.at[k], partner
        )

    def p_copy(k):
        origin = lax.rem(g - k + groups, groups)
        return remote(
            spill_res.at[1, origin], spill_part.at[origin], ps_sem.at[k], pr_sem.at[k], partner
        )

    def c_copy(k):
        origin = lax.rem(g - k + groups, groups)
        return remote(
            spill_comb.at[origin], spill_ret.at[g], cs_sem.at[k], cr_sem.at[k], 2 * origin + p
        )

    def r_copy(k):
        origin = lax.rem(e - k + experts, experts)
        return remote(home_res.at[origin], home_ret.at[e], rs_sem.at[k], rr_sem.at[k], origin)

    @pl.loop(1, groups)
    def _(k):
        z_copy(k).start()

    @pl.loop(1, experts)
    def _(k):
        h_copy(k).start()

    for copy in own:
        copy.wait()
    x_copy(0).start()

    tok = tok_ref[...]
    shared_gate = jnp.dot(tok, sg_ref[...], preferred_element_type=jnp.float32)
    shared_up = jnp.dot(tok, su_ref[...], preferred_element_type=jnp.float32)
    shared_ref[...] = (jax.nn.silu(shared_gate) * shared_up).astype(jnp.bfloat16)

    for copy in weights:
        copy.wait()

    def ffn(x):
        gate_out = jnp.dot(x, wg[...], preferred_element_type=jnp.float32)
        up_out = jnp.dot(x, wu[...], preferred_element_type=jnp.float32)
        hidden = (jax.nn.silu(gate_out) * up_out).astype(jnp.bfloat16)
        return jnp.dot(hidden, wd[...], preferred_element_type=jnp.float32).astype(jnp.bfloat16)

    @pl.loop(1, groups)
    def _(k):
        z_copy(k).wait_recv()
        x_copy(k).start()

    @pl.loop(0, experts)
    def _(k):
        origin = lax.rem(e - k + experts, experts)

        @pl.when(k > 0)
        def _():
            h_copy(k).wait_recv()

        home_res[origin] = ffn(home_in[origin])

        @pl.when(k > 0)
        def _():
            r_copy(k).start()

    own_ret = pltpu.make_async_copy(home_res.at[e], home_ret.at[e], own_sem.at[0])
    own_ret.start()

    @pl.loop(0, groups)
    def _(k):
        origin = lax.rem(g - k + groups, groups)
        x_copy(k).wait_recv()
        spill_res[1, origin] = ffn(spill_in[1, origin])
        p_copy(k).start()

    @pl.loop(0, groups)
    def _(k):
        origin = lax.rem(g - k + groups, groups)
        mine = ffn(spill_in[0, origin])
        p_copy(k).wait_recv()
        spill_comb[origin] = jnp.where(mask_ref[origin][:, :1] > 0.5, mine, spill_part[origin])

        @pl.when(k > 0)
        def _():
            c_copy(k).start()

    own_back = pltpu.make_async_copy(spill_comb.at[g], spill_ret.at[g], own_sem.at[1])
    own_back.start()

    @pl.loop(0, groups)
    def _(k):
        x_copy(k).wait_send()
        p_copy(k).wait_send()

    @pl.loop(1, groups)
    def _(k):
        z_copy(k).wait_send()
        c_copy(k).wait()

    @pl.loop(1, experts)
    def _(k):
        h_copy(k).wait_send()
        r_copy(k).wait()

    own_ret.wait()
    own_back.wait()


def routed_exchange(home_out, spill_out, mask, tokens, w_gate, w_up, w_down, shared_gate, shared_up):
    experts, home, width = home_out.shape
    groups, extra, _ = spill_out.shape
    bf16 = jnp.bfloat16
    vmem = pl.BlockSpec(memory_space=pltpu.VMEM)
    anywhere = pl.BlockSpec(memory_space=pl.ANY)
    dma = pltpu.SemaphoreType.DMA
    return pl.pallas_call(
        functools.partial(moe_kernel, experts, groups),
        out_shape=(
            jax.ShapeDtypeStruct(home_out.shape, bf16),
            jax.ShapeDtypeStruct(spill_out.shape, bf16),
            jax.ShapeDtypeStruct((tokens.shape[0], shared_gate.shape[1]), bf16),
        ),
        in_specs=[vmem] * 4 + [anywhere] * 3 + [vmem] * 2,
        out_specs=(vmem, vmem, vmem),
        scratch_shapes=[
            pltpu.VMEM(home_out.shape, bf16),
            pltpu.VMEM(home_out.shape, bf16),
            pltpu.VMEM((2,) + spill_out.shape, bf16),
            pltpu.VMEM((2,) + spill_out.shape, bf16),
            pltpu.VMEM(spill_out.shape, bf16),
            pltpu.VMEM(spill_out.shape, bf16),
            pltpu.VMEM(w_gate.shape, bf16),
            pltpu.VMEM(w_up.shape, bf16),
            pltpu.VMEM(w_down.shape, bf16),
            dma((3,)),
            dma((2,)),
        ]
        + [dma((experts,))] * 4
        + [dma((groups,))] * 8,
        compiler_params=pltpu.CompilerParams(
            has_side_effects=True, vmem_limit_bytes=60 * 1024 * 1024
        ),
        name=f"moe{extra}",
    )(home_out, spill_out, mask, tokens, w_gate, w_up, w_down, shared_gate, shared_up)


def body(
    tokens,
    router_logit,
    expert_id,
    token_slot,
    keep,
    overflow_host,
    expert_gate,
    expert_up,
    expert_down,
    shared_gate,
    shared_up,
    shared_down,
):
    experts = lax.axis_size("expert")
    dps = lax.axis_size("dp")
    groups = experts // 2
    my_e = lax.axis_index("expert")
    tok_count, model_width = tokens.shape
    slot_count = 2 * tok_count // experts
    home_count = slot_count // 2
    spill_count = slot_count - home_count
    w_gate, w_up, w_down = expert_gate[0], expert_up[0], expert_down[0]
    token_scale = jax.nn.sigmoid(router_logit) * keep.astype(jnp.float32)
    routed_in = (tokens.astype(jnp.float32) * token_scale[:, None]).astype(jnp.bfloat16)
    positions = jnp.arange(tok_count, dtype=jnp.int32)
    is_spill = token_slot >= home_count
    spill_level = jnp.maximum(token_slot - home_count, 0)
    table_index = expert_id * spill_count + spill_level
    table_ids = jnp.arange(experts * spill_count, dtype=jnp.int32)
    host_expert = jnp.sum(
        jnp.where(table_index[:, None] == table_ids[None, :], overflow_host.reshape(1, -1), 0),
        axis=1,
    )
    host_group, host_side = host_expert // 2, host_expert % 2
    spill_key = jnp.where(is_spill, host_group, -1 - positions)
    earlier = (spill_key[:, None] == spill_key[None, :]) & (positions[None, :] < positions[:, None])
    spill_rank = jnp.sum(earlier.astype(jnp.int32), axis=1)
    need = jnp.max(jnp.where(is_spill, spill_rank + 1, 0))

    most = 2 * slot_count
    levels = [max(1, most * part // 16) for part in (3, 4)]
    lanes_max = 128
    meta_rows = max(8, groups)
    fits = is_spill & (spill_rank < lanes_max)
    meta_cell = jnp.where(fits, host_group * lanes_max + spill_rank, -1)
    meta_ids = jnp.arange(meta_rows * lanes_max, dtype=jnp.int32)
    side_at = jnp.sum(jnp.where(meta_ids[:, None] == meta_cell[None, :], host_side[None, :], 0), axis=1)
    meta = (2 * need + side_at).reshape(meta_rows, lanes_max).astype(jnp.int32)
    everyone = gather_meta(meta)
    need = jnp.max(everyone) // 2
    by_source = everyone.reshape(dps, groups, 2, meta_rows, lanes_max)
    column = by_source[lax.axis_index("dp"), :, my_e % 2, my_e // 2, :]
    mine = ((column % 2) == my_e % 2).astype(jnp.float32)

    def shared_part():
        return (
            jax.nn.silu(jnp.dot(tokens, shared_gate, preferred_element_type=jnp.float32))
            * jnp.dot(tokens, shared_up, preferred_element_type=jnp.float32)
        ).astype(jnp.bfloat16)

    def short(extra):
        def run(rows):
            home_cell = jnp.where(is_spill, -1, expert_id * home_count + token_slot)
            spill_cell = jnp.where(is_spill, host_group * extra + spill_rank, -1)
            home_ids = jnp.arange(experts * home_count, dtype=jnp.int32)
            spill_ids = jnp.arange(groups * extra, dtype=jnp.int32)
            home_pick = (home_ids[:, None] == home_cell[None, :]).astype(jnp.bfloat16)
            spill_pick = (spill_ids[:, None] == spill_cell[None, :]).astype(jnp.bfloat16)
            home_out = jnp.dot(home_pick, rows, preferred_element_type=jnp.float32).astype(jnp.bfloat16)
            spill_out = jnp.dot(spill_pick, rows, preferred_element_type=jnp.float32).astype(jnp.bfloat16)
            mask = jnp.broadcast_to(mine[:, :extra, None], (groups, extra, 128))
            home_ret, spill_ret, shared_hidden = routed_exchange(
                home_out.reshape(experts, home_count, model_width),
                spill_out.reshape(groups, extra, model_width),
                mask,
                tokens,
                w_gate,
                w_up,
                w_down,
                shared_gate,
                shared_up,
            )
            pick = jnp.concatenate([home_pick.T, spill_pick.T, shared_hidden], axis=1)
            source = jnp.concatenate(
                [
                    home_ret.reshape(-1, model_width),
                    spill_ret.reshape(-1, model_width),
                    shared_down,
                ],
                axis=0,
            )
            return jnp.dot(pick, source, preferred_element_type=jnp.float32).astype(jnp.bfloat16)

        return run

    def whole(rows):
        lanes = home_count + 2 * spill_count
        to_right = host_expert == (expert_id + 1) % experts
        lane_index = jnp.where(
            is_spill,
            home_count + spill_level + jnp.where(to_right, 0, spill_count),
            token_slot,
        )
        cell_index = jnp.where(is_spill, host_expert, expert_id) * lanes + lane_index
        source_row = jnp.zeros((experts * lanes,), jnp.int32).at[cell_index].set(positions)
        outgoing = rows[source_row].reshape(experts, lanes, model_width)
        incoming = lax.all_to_all(outgoing, "expert", split_axis=0, concat_axis=0, tiled=True)
        answers = lax.all_to_all(
            expert_ffn(incoming, w_gate, w_up, w_down),
            "expert",
            split_axis=0,
            concat_axis=0,
            tiled=True,
        )
        routed = answers.reshape(-1, model_width)[cell_index]
        shared_out = jnp.dot(shared_part(), shared_down, preferred_element_type=jnp.float32)
        return (shared_out + routed.astype(jnp.float32)).astype(jnp.bfloat16)

    chosen = sum((need > level).astype(jnp.int32) for level in levels)
    return lax.switch(chosen, [short(level) for level in levels] + [whole], routed_in)


def solution(mesh):
    return jax.shard_map(
        body,
        mesh=mesh,
        in_specs=(
            P(("dp", "expert"), None),
            P(("dp", "expert")),
            P(("dp", "expert")),
            P(("dp", "expert")),
            P(("dp", "expert")),
            P(),
            P("expert", None, None),
            P("expert", None, None),
            P("expert", None, None),
            P(),
            P(),
            P(),
        ),
        out_specs=P(("dp", "expert"), None),
        check_vma=False,
    )
```

```python
import functools

import jax
import jax.numpy as jnp
from jax import lax
from jax.experimental import pallas as pl
from jax.experimental.pallas import tpu as pltpu
from jax.sharding import PartitionSpec as P

MESH = pl.DeviceIdType.MESH


def expert_ffn(inputs, w_gate, w_up, w_down):
    flat_rows = inputs.reshape(-1, inputs.shape[-1])
    gate_out = jnp.dot(flat_rows, w_gate, preferred_element_type=jnp.float32)
    up_out = jnp.dot(flat_rows, w_up, preferred_element_type=jnp.float32)
    hidden = (jax.nn.silu(gate_out) * up_out).astype(jnp.bfloat16)
    result = jnp.dot(hidden, w_down, preferred_element_type=jnp.float32).astype(jnp.bfloat16)
    return result.reshape(inputs.shape)


def flip(index, step, count):
    out, bit = 0, 1
    while bit < count:
        out = out + bit * lax.rem(index // bit + step // bit, 2)
        bit *= 2
    return out


def moe_kernel(
    dps,
    experts,
    groups,
    home_out,
    pool_out,
    side_out,
    need_ref,
    tok_ref,
    wg_hbm,
    wu_hbm,
    wd_hbm,
    sg_ref,
    su_ref,
    home_ret,
    pool_ret,
    shared_ref,
    need_all,
    home_in,
    home_res,
    pool_in,
    pool_res,
    pool_part,
    pool_comb,
    side_in,
    wg,
    wu,
    wd,
    w_sem,
    own_sem,
    ns_sem,
    nr_sem,
    hs_sem,
    hr_sem,
    rs_sem,
    rr_sem,
    zs_sem,
    zr_sem,
    ms_sem,
    mr_sem,
    xs_sem,
    xr_sem,
    ps_sem,
    pr_sem,
    cs_sem,
    cr_sem,
):
    my_dp = lax.axis_index("dp")
    e = lax.axis_index("expert")
    g = e // 2
    p = e - 2 * g
    partner = e + 1 - 2 * p
    total = dps * experts
    me = my_dp * experts + e

    weights = [
        pltpu.make_async_copy(a, b, w_sem.at[i])
        for i, (a, b) in enumerate(((wg_hbm, wg), (wu_hbm, wu), (wd_hbm, wd)))
    ]
    own = [
        pltpu.make_async_copy(home_out.at[e], home_in.at[e], own_sem.at[0]),
        pltpu.make_async_copy(pool_out.at[g], pool_in.at[0, g], own_sem.at[1]),
        pltpu.make_async_copy(side_out.at[g], side_in.at[g], own_sem.at[2]),
        pltpu.make_async_copy(need_ref, need_all.at[me], own_sem.at[3]),
    ]

    def remote(src, dst, send, recv, to):
        return pltpu.make_async_remote_copy(
            src_ref=src,
            dst_ref=dst,
            send_sem=send,
            recv_sem=recv,
            device_id={"expert": to},
            device_id_type=MESH,
        )

    def n_copy(k):
        there = lax.rem(me + k, total)
        return pltpu.make_async_remote_copy(
            src_ref=need_ref,
            dst_ref=need_all.at[me],
            send_sem=ns_sem.at[k],
            recv_sem=nr_sem.at[k],
            device_id={"dp": there // experts, "expert": lax.rem(there, experts)},
            device_id_type=MESH,
        )

    def z_copy(k):
        to = flip(g, k, groups)
        return remote(pool_out.at[to], pool_in.at[0, g], zs_sem.at[k], zr_sem.at[k], 2 * to + p)

    def m_copy(k):
        to = flip(g, k, groups)
        return remote(side_out.at[to], side_in.at[g], ms_sem.at[k], mr_sem.at[k], 2 * to + p)

    def h_copy(k):
        to = flip(e, k, experts)
        return remote(home_out.at[to], home_in.at[e], hs_sem.at[k], hr_sem.at[k], to)

    def x_copy(k):
        origin = flip(g, k, groups)
        return remote(
            pool_in.at[0, origin],
            pool_in.at[1, flip(g, k, groups)],
            xs_sem.at[k],
            xr_sem.at[k],
            partner,
        )

    def p_copy(k):
        origin = flip(g, k, groups)
        return remote(
            pool_res.at[origin], pool_part.at[origin], ps_sem.at[k], pr_sem.at[k], partner
        )

    def c_copy(k):
        origin = flip(g, k, groups)
        return remote(
            pool_comb.at[origin], pool_ret.at[g], cs_sem.at[k], cr_sem.at[k], 2 * origin + p
        )

    def r_copy(k):
        origin = flip(e, k, experts)
        return remote(home_res.at[origin], home_ret.at[e], rs_sem.at[k], rr_sem.at[k], origin)

    @pl.loop(1, groups)
    def _(i):
        z_copy(groups - i).start()
        m_copy(groups - i).start()

    @pl.loop(1, experts)
    def _(i):
        h_copy(experts - i).start()

    for copy in own:
        copy.start()
    for copy in weights:
        copy.start()

    @pl.loop(1, total)
    def _(k):
        n_copy(k).start()

    for copy in own:
        copy.wait()
    x_copy(0).start()

    tok = tok_ref[...]
    last = (((1,), (1,)), ((), ()))
    shared_gate = lax.dot_general(tok, sg_ref[...], last, preferred_element_type=jnp.float32)
    shared_up = lax.dot_general(tok, su_ref[...], last, preferred_element_type=jnp.float32)
    shared_ref[...] = (jax.nn.silu(shared_gate) * shared_up).astype(jnp.bfloat16)

    for copy in weights:
        copy.wait()

    def ffn(x):
        gate_out = jnp.dot(x, wg[...], preferred_element_type=jnp.float32)
        up_out = jnp.dot(x, wu[...], preferred_element_type=jnp.float32)
        hidden = (jax.nn.silu(gate_out) * up_out).astype(jnp.bfloat16)
        return jnp.dot(hidden, wd[...], preferred_element_type=jnp.float32).astype(jnp.bfloat16)

    home_res[e] = ffn(home_in[e])
    own_ret = pltpu.make_async_copy(home_res.at[e], home_ret.at[e], own_sem.at[0])
    own_ret.start()

    @pl.loop(1, groups)
    def _(i):
        k = groups - i
        z_copy(k).wait_recv()
        x_copy(k).start()

    def home_block(i):
        k = experts - i
        origin = flip(e, k, experts)
        h_copy(k).wait_recv()
        home_res[origin] = ffn(home_in[origin])
        r_copy(k).start()

    half = experts // 2 + 1
    pl.loop(1, half)(home_block)

    @pl.loop(1, groups + 1)
    def _(i):
        k = groups - i
        origin = flip(g, k, groups)
        x_copy(k).wait_recv()
        pool_res[origin] = ffn(pool_in[1, origin])
        p_copy(k).start()

    @pl.loop(1, groups + 1)
    def _(i):
        k = groups - i
        origin = flip(g, k, groups)
        mine = ffn(pool_in[0, origin])
        p_copy(k).wait_recv()

        @pl.when(k > 0)
        def _():
            m_copy(k).wait_recv()

        here = jnp.abs(side_in[origin][:, :1] - p.astype(jnp.float32)) < 0.5
        pool_comb[origin] = jnp.where(here, mine, pool_part[origin])

        @pl.when(k > 0)
        def _():
            c_copy(k).start()

    own_back = pltpu.make_async_copy(pool_comb.at[g], pool_ret.at[g], own_sem.at[1])
    own_back.start()

    pl.loop(half, experts)(home_block)

    @pl.loop(0, groups)
    def _(k):
        x_copy(k).wait_send()
        p_copy(k).wait_send()

    @pl.loop(1, groups)
    def _(k):
        z_copy(k).wait_send()
        m_copy(k).wait_send()
        c_copy(k).wait()

    @pl.loop(1, total)
    def _(k):
        n_copy(k).wait()

    @pl.loop(1, experts)
    def _(k):
        h_copy(k).wait_send()
        r_copy(k).wait()

    own_ret.wait()
    own_back.wait()


def routed_exchange(
    home_out, pool_out, side_out, need, tokens, w_gate, w_up, w_down, shared_gate, shared_up
):
    dps, experts = lax.axis_size("dp"), lax.axis_size("expert")
    groups = pool_out.shape[0]
    bf16 = jnp.bfloat16
    vmem = pl.BlockSpec(memory_space=pltpu.VMEM)
    anywhere = pl.BlockSpec(memory_space=pl.ANY)
    dma = pltpu.SemaphoreType.DMA
    return pl.pallas_call(
        functools.partial(moe_kernel, dps, experts, groups),
        out_shape=(
            jax.ShapeDtypeStruct(home_out.shape, bf16),
            jax.ShapeDtypeStruct(pool_out.shape, bf16),
            jax.ShapeDtypeStruct((tokens.shape[0], shared_gate.shape[0]), bf16),
            jax.ShapeDtypeStruct((dps * experts,) + need.shape, need.dtype),
        ),
        in_specs=[vmem] * 5 + [anywhere] * 3 + [vmem] * 2,
        out_specs=(vmem,) * 4,
        scratch_shapes=[
            pltpu.VMEM(home_out.shape, bf16),
            pltpu.VMEM(home_out.shape, bf16),
            pltpu.VMEM((2,) + pool_out.shape, bf16),
            pltpu.VMEM(pool_out.shape, bf16),
            pltpu.VMEM(pool_out.shape, bf16),
            pltpu.VMEM(pool_out.shape, bf16),
            pltpu.VMEM(side_out.shape, jnp.float32),
            pltpu.VMEM(w_gate.shape, bf16),
            pltpu.VMEM(w_up.shape, bf16),
            pltpu.VMEM(w_down.shape, bf16),
            dma((3,)),
            dma((4,)),
        ]
        + [dma((dps * experts,))] * 2
        + [dma((experts,))] * 4
        + [dma((groups,))] * 10,
        compiler_params=pltpu.CompilerParams(
            has_side_effects=True, vmem_limit_bytes=60 * 1024 * 1024
        ),
        name="moe",
    )(home_out, pool_out, side_out, need, tokens, w_gate, w_up, w_down, shared_gate, shared_up)


def body(
    tokens,
    router_logit,
    expert_id,
    token_slot,
    keep,
    overflow_host,
    expert_gate,
    expert_up,
    expert_down,
    shared_gate,
    shared_up,
    shared_down,
):
    experts = lax.axis_size("expert")
    dps = lax.axis_size("dp")
    groups = experts // 2
    my_e = lax.axis_index("expert")
    tok_count, model_width = tokens.shape
    slot_count = 2 * tok_count // experts
    home_count = slot_count // 2
    spill_count = slot_count - home_count
    w_gate, w_up, w_down = expert_gate[0], expert_up[0], expert_down[0]
    token_scale = jax.nn.sigmoid(router_logit) * keep.astype(jnp.float32)
    routed_in = (tokens.astype(jnp.float32) * token_scale[:, None]).astype(jnp.bfloat16)
    positions = jnp.arange(tok_count, dtype=jnp.int32)
    is_spill = token_slot >= home_count
    spill_level = jnp.maximum(token_slot - home_count, 0)
    table_index = expert_id * spill_count + spill_level
    table_ids = jnp.arange(experts * spill_count, dtype=jnp.int32)
    host_expert = jnp.sum(
        jnp.where(table_index[:, None] == table_ids[None, :], overflow_host.reshape(1, -1), 0),
        axis=1,
    )
    served = jnp.where(is_spill, host_expert, expert_id)
    kept = keep != 0
    before = positions[None, :] < positions[:, None]

    def rank_of(member, label):
        same = (label[:, None] == label[None, :]) & member[None, :] & before
        return jnp.sum(same.astype(jnp.int32), axis=1)

    direct = max(1, 3 * home_count // 4)
    pooled = home_count
    direct_rank = rank_of(kept, served)
    over = kept & (direct_rank >= direct)
    pool_rank = rank_of(over, served // 2)
    left = over & (pool_rank >= pooled)
    home_cell = jnp.where(kept & ~over, served * direct + direct_rank, -1)
    pool_cell = jnp.where(over & ~left, (served // 2) * pooled + pool_rank, -1)
    home_ids = jnp.arange(experts * direct, dtype=jnp.int32)
    pool_ids = jnp.arange(groups * pooled, dtype=jnp.int32)
    home_pick = (home_ids[:, None] == home_cell[None, :]).astype(jnp.bfloat16)
    pool_pick = (pool_ids[:, None] == pool_cell[None, :]).astype(jnp.bfloat16)
    home_out = jnp.dot(home_pick, routed_in, preferred_element_type=jnp.float32).astype(jnp.bfloat16)
    pool_out = jnp.dot(pool_pick, routed_in, preferred_element_type=jnp.float32).astype(jnp.bfloat16)
    side = jnp.sum(
        jnp.where(pool_ids[:, None] == pool_cell[None, :], (served % 2)[None, :], 0), axis=1
    )
    side_out = jnp.broadcast_to(side.astype(jnp.float32)[:, None], (groups * pooled, 128))
    unserved = jnp.broadcast_to(jnp.max(left.astype(jnp.int32)), (8, 128))
    home_ret, pool_ret, shared_hidden, unserved_all = routed_exchange(
        home_out.reshape(experts, direct, model_width),
        pool_out.reshape(groups, pooled, model_width),
        side_out.reshape(groups, pooled, 128),
        unserved,
        tokens,
        w_gate,
        w_up,
        w_down,
        shared_gate.T,
        shared_up.T,
    )

    def combined():
        home_back = (home_cell[:, None] == home_ids[None, :]).astype(jnp.bfloat16)
        pool_back = (pool_cell[:, None] == pool_ids[None, :]).astype(jnp.bfloat16)
        pick = jnp.concatenate([home_back, pool_back, shared_hidden], axis=1)
        source = jnp.concatenate(
            [home_ret.reshape(-1, model_width), pool_ret.reshape(-1, model_width), shared_down],
            axis=0,
        )
        return jnp.dot(pick, source, preferred_element_type=jnp.float32)

    def all_served(rows):
        return combined().astype(jnp.bfloat16)

    def some_left(rows):
        lanes = home_count + 2 * spill_count
        to_right = host_expert == (expert_id + 1) % experts
        lane_index = jnp.where(
            is_spill,
            home_count + spill_level + jnp.where(to_right, 0, spill_count),
            token_slot,
        )
        cell_index = served * lanes + lane_index
        source_row = jnp.zeros((experts * lanes,), jnp.int32).at[cell_index].set(positions)
        outgoing = rows[source_row].reshape(experts, lanes, model_width)
        incoming = lax.all_to_all(outgoing, "expert", split_axis=0, concat_axis=0, tiled=True)
        answers = lax.all_to_all(
            expert_ffn(incoming, w_gate, w_up, w_down),
            "expert",
            split_axis=0,
            concat_axis=0,
            tiled=True,
        )
        rest = answers.reshape(-1, model_width)[cell_index].astype(jnp.float32)
        return (combined() + jnp.where(left[:, None], rest, 0.0)).astype(jnp.bfloat16)

    return lax.cond(jnp.max(unserved_all) > 0, some_left, all_served, routed_in)


def solution(mesh):
    return jax.shard_map(
        body,
        mesh=mesh,
        in_specs=(
            P(("dp", "expert"), None),
            P(("dp", "expert")),
            P(("dp", "expert")),
            P(("dp", "expert")),
            P(("dp", "expert")),
            P(),
            P("expert", None, None),
            P("expert", None, None),
            P("expert", None, None),
            P(),
            P(),
            P(),
        ),
        out_specs=P(("dp", "expert"), None),
        check_vma=False,
    )
```

```python
import functools

import jax
import jax.numpy as jnp
from jax import lax
from jax.experimental import pallas as pl
from jax.experimental.pallas import tpu as pltpu
from jax.sharding import PartitionSpec as P

MESH = pl.DeviceIdType.MESH


def expert_ffn(inputs, w_gate, w_up, w_down):
    flat_rows = inputs.reshape(-1, inputs.shape[-1])
    gate_out = jnp.dot(flat_rows, w_gate, preferred_element_type=jnp.float32)
    up_out = jnp.dot(flat_rows, w_up, preferred_element_type=jnp.float32)
    hidden = (jax.nn.silu(gate_out) * up_out).astype(jnp.bfloat16)
    result = jnp.dot(hidden, w_down, preferred_element_type=jnp.float32).astype(jnp.bfloat16)
    return result.reshape(inputs.shape)


def flip(index, step, count):
    out, bit = 0, 1
    while bit < count:
        out = out + bit * lax.rem(index // bit + step // bit, 2)
        bit *= 2
    return out


def moe_kernel(
    dps,
    experts,
    groups,
    home_pick,
    pool_pick,
    side_out,
    need_ref,
    scale_ref,
    tok_ref,
    wg_hbm,
    wu_hbm,
    wd_hbm,
    sg_ref,
    su_ref,
    home_ret,
    pool_ret,
    shared_ref,
    need_max,
    need_all,
    routed_in,
    home_out,
    pool_out,
    home_in,
    home_res,
    pool_in,
    pool_res,
    pool_part,
    pool_comb,
    side_in,
    wg,
    wu,
    wd,
    w_sem,
    own_sem,
    ns_sem,
    nr_sem,
    hs_sem,
    hr_sem,
    rs_sem,
    rr_sem,
    zs_sem,
    zr_sem,
    ms_sem,
    mr_sem,
    xs_sem,
    xr_sem,
    ps_sem,
    pr_sem,
    cs_sem,
    cr_sem,
):
    my_dp = lax.axis_index("dp")
    e = lax.axis_index("expert")
    g = e // 2
    p = e - 2 * g
    partner = e + 1 - 2 * p
    total = dps * experts
    me = my_dp * experts + e

    weights = [
        pltpu.make_async_copy(a, b, w_sem.at[i])
        for i, (a, b) in enumerate(((wg_hbm, wg), (wu_hbm, wu), (wd_hbm, wd)))
    ]
    own = [
        pltpu.make_async_copy(home_out.at[e], home_in.at[e], own_sem.at[0]),
        pltpu.make_async_copy(pool_out.at[g], pool_in.at[0, g], own_sem.at[1]),
        pltpu.make_async_copy(side_out.at[g], side_in.at[g], own_sem.at[2]),
        pltpu.make_async_copy(need_ref, need_all.at[me], own_sem.at[3]),
    ]

    def remote(src, dst, send, recv, to):
        return pltpu.make_async_remote_copy(
            src_ref=src,
            dst_ref=dst,
            send_sem=send,
            recv_sem=recv,
            device_id={"expert": to},
            device_id_type=MESH,
        )

    def n_copy(k):
        there = lax.rem(me + k, total)
        return pltpu.make_async_remote_copy(
            src_ref=need_ref,
            dst_ref=need_all.at[me],
            send_sem=ns_sem.at[k],
            recv_sem=nr_sem.at[k],
            device_id={"dp": there // experts, "expert": lax.rem(there, experts)},
            device_id_type=MESH,
        )

    def z_copy(k):
        to = flip(g, k, groups)
        return remote(pool_out.at[to], pool_in.at[0, g], zs_sem.at[k], zr_sem.at[k], 2 * to + p)

    def m_copy(k):
        to = flip(g, k, groups)
        return remote(side_out.at[to], side_in.at[g], ms_sem.at[k], mr_sem.at[k], 2 * to + p)

    def h_copy(k):
        to = flip(e, k, experts)
        return remote(home_out.at[to], home_in.at[e], hs_sem.at[k], hr_sem.at[k], to)

    def x_copy(k):
        origin = flip(g, k, groups)
        return remote(
            pool_in.at[0, origin],
            pool_in.at[1, flip(g, k, groups)],
            xs_sem.at[k],
            xr_sem.at[k],
            partner,
        )

    def p_copy(k):
        origin = flip(g, k, groups)
        return remote(
            pool_res.at[origin], pool_part.at[origin], ps_sem.at[k], pr_sem.at[k], partner
        )

    def c_copy(k):
        origin = flip(g, k, groups)
        return remote(
            pool_comb.at[origin], pool_ret.at[g], cs_sem.at[k], cr_sem.at[k], 2 * origin + p
        )

    def r_copy(k):
        origin = flip(e, k, experts)
        return remote(home_res.at[origin], home_ret.at[e], rs_sem.at[k], rr_sem.at[k], origin)

    def rows_of(pick):
        return jnp.dot(pick, routed_in[...], preferred_element_type=jnp.float32).astype(jnp.bfloat16)

    routed_in[...] = (tok_ref[...].astype(jnp.float32) * scale_ref[...]).astype(jnp.bfloat16)

    @pl.loop(1, groups + 1)
    def _(i):
        k = groups - i
        to = flip(g, k, groups)
        pool_out[to] = rows_of(pool_pick[to])

        @pl.when(i > 1)
        def _():
            z_copy(k + 1).start()
            m_copy(k + 1).start()

    @pl.loop(1, experts + 1)
    def _(i):
        k = experts - i
        to = flip(e, k, experts)
        home_out[to] = rows_of(home_pick[to])

        @pl.when(i > 1)
        def _():
            h_copy(k + 1).start()

    for copy in own:
        copy.start()
    for copy in weights:
        copy.start()

    @pl.loop(1, total)
    def _(k):
        n_copy(k).start()

    for copy in own:
        copy.wait()
    x_copy(0).start()

    tok = tok_ref[...]
    last = (((1,), (1,)), ((), ()))
    shared_gate = lax.dot_general(tok, sg_ref[...], last, preferred_element_type=jnp.float32)
    shared_up = lax.dot_general(tok, su_ref[...], last, preferred_element_type=jnp.float32)
    shared_ref[...] = (jax.nn.silu(shared_gate) * shared_up).astype(jnp.bfloat16)

    for copy in weights:
        copy.wait()

    def ffn(x):
        gate_out = jnp.dot(x, wg[...], preferred_element_type=jnp.float32)
        up_out = jnp.dot(x, wu[...], preferred_element_type=jnp.float32)
        hidden = (jax.nn.silu(gate_out) * up_out).astype(jnp.bfloat16)
        return jnp.dot(hidden, wd[...], preferred_element_type=jnp.float32).astype(jnp.bfloat16)

    home_res[e] = ffn(home_in[e])
    own_ret = pltpu.make_async_copy(home_res.at[e], home_ret.at[e], own_sem.at[0])
    own_ret.start()

    @pl.loop(1, groups)
    def _(i):
        k = groups - i
        z_copy(k).wait_recv()
        x_copy(k).start()

    def home_block(i):
        k = experts - i
        origin = flip(e, k, experts)
        h_copy(k).wait_recv()
        home_res[origin] = ffn(home_in[origin])
        r_copy(k).start()

    @pl.loop(1, groups + 1)
    def _(i):
        k = groups - i
        origin = flip(g, k, groups)
        x_copy(k).wait_recv()
        pool_res[origin] = ffn(pool_in[1, origin])
        p_copy(k).start()

    @pl.loop(1, groups + 1)
    def _(i):
        k = groups - i
        origin = flip(g, k, groups)
        mine = ffn(pool_in[0, origin])
        p_copy(k).wait_recv()

        @pl.when(k > 0)
        def _():
            m_copy(k).wait_recv()

        here = jnp.abs(side_in[origin][:, :1] - p.astype(jnp.float32)) < 0.5
        pool_comb[origin] = jnp.where(here, mine, pool_part[origin])

        @pl.when(k > 0)
        def _():
            c_copy(k).start()

    own_back = pltpu.make_async_copy(pool_comb.at[g], pool_ret.at[g], own_sem.at[1])
    own_back.start()

    pl.loop(1, experts)(home_block)

    @pl.loop(0, groups)
    def _(k):
        x_copy(k).wait_send()
        p_copy(k).wait_send()

    @pl.loop(1, groups)
    def _(k):
        z_copy(k).wait_send()
        m_copy(k).wait_send()
        c_copy(k).wait()

    @pl.loop(1, total)
    def _(k):
        n_copy(k).wait()

    @pl.loop(1, experts)
    def _(k):
        h_copy(k).wait_send()
        r_copy(k).wait()

    own_ret.wait()
    own_back.wait()
    need_max[...] = jnp.max(need_all[...], axis=0)


def routed_exchange(
    home_pick, pool_pick, side_out, need, scale, tokens, w_gate, w_up, w_down, shared_gate, shared_up
):
    dps, experts = lax.axis_size("dp"), lax.axis_size("expert")
    groups = pool_pick.shape[0]
    width = tokens.shape[1]
    home_shape, pool_shape = home_pick.shape[:2] + (width,), pool_pick.shape[:2] + (width,)
    bf16 = jnp.bfloat16
    vmem = pl.BlockSpec(memory_space=pltpu.VMEM)
    anywhere = pl.BlockSpec(memory_space=pl.ANY)
    dma = pltpu.SemaphoreType.DMA
    return pl.pallas_call(
        functools.partial(moe_kernel, dps, experts, groups),
        out_shape=(
            jax.ShapeDtypeStruct(home_shape, bf16),
            jax.ShapeDtypeStruct(pool_shape, bf16),
            jax.ShapeDtypeStruct((tokens.shape[0], shared_gate.shape[0]), bf16),
            jax.ShapeDtypeStruct(need.shape, need.dtype),
        ),
        in_specs=[vmem] * 6 + [anywhere] * 3 + [vmem] * 2,
        out_specs=(vmem,) * 4,
        scratch_shapes=[
            pltpu.VMEM((dps * experts,) + need.shape, need.dtype),
            pltpu.VMEM(tokens.shape, bf16),
            pltpu.VMEM(home_shape, bf16),
            pltpu.VMEM(pool_shape, bf16),
            pltpu.VMEM(home_shape, bf16),
            pltpu.VMEM(home_shape, bf16),
            pltpu.VMEM((2,) + pool_shape, bf16),
            pltpu.VMEM(pool_shape, bf16),
            pltpu.VMEM(pool_shape, bf16),
            pltpu.VMEM(pool_shape, bf16),
            pltpu.VMEM(side_out.shape, jnp.float32),
            pltpu.VMEM(w_gate.shape, bf16),
            pltpu.VMEM(w_up.shape, bf16),
            pltpu.VMEM(w_down.shape, bf16),
            dma((3,)),
            dma((4,)),
        ]
        + [dma((dps * experts,))] * 2
        + [dma((experts,))] * 4
        + [dma((groups,))] * 10,
        compiler_params=pltpu.CompilerParams(
            has_side_effects=True, vmem_limit_bytes=60 * 1024 * 1024
        ),
        name="moe",
    )(home_pick, pool_pick, side_out, need, scale, tokens, w_gate, w_up, w_down, shared_gate, shared_up)


def body(
    tokens,
    router_logit,
    expert_id,
    token_slot,
    keep,
    overflow_host,
    expert_gate,
    expert_up,
    expert_down,
    shared_gate,
    shared_up,
    shared_down,
):
    experts = lax.axis_size("expert")
    dps = lax.axis_size("dp")
    groups = experts // 2
    my_e = lax.axis_index("expert")
    tok_count, model_width = tokens.shape
    slot_count = 2 * tok_count // experts
    home_count = slot_count // 2
    spill_count = slot_count - home_count
    w_gate, w_up, w_down = expert_gate[0], expert_up[0], expert_down[0]
    token_scale = jax.nn.sigmoid(router_logit) * keep.astype(jnp.float32)
    positions = jnp.arange(tok_count, dtype=jnp.int32)
    is_spill = token_slot >= home_count
    spill_level = jnp.maximum(token_slot - home_count, 0)
    table_index = expert_id * spill_count + spill_level
    table_ids = jnp.arange(experts * spill_count, dtype=jnp.int32)
    host_expert = jnp.sum(
        jnp.where(table_index[:, None] == table_ids[None, :], overflow_host.reshape(1, -1), 0),
        axis=1,
    )
    served = jnp.where(is_spill, host_expert, expert_id)
    kept = keep != 0
    before = positions[None, :] < positions[:, None]

    def rank_of(member, label):
        same = (label[:, None] == label[None, :]) & member[None, :] & before
        return jnp.sum(same.astype(jnp.int32), axis=1)

    direct = max(1, 3 * home_count // 4)
    pooled = home_count
    direct_rank = rank_of(kept, served)
    over = kept & (direct_rank >= direct)
    pool_rank = rank_of(over, served // 2)
    left = over & (pool_rank >= pooled)
    home_cell = jnp.where(kept & ~over, served * direct + direct_rank, -1)
    pool_cell = jnp.where(over & ~left, (served // 2) * pooled + pool_rank, -1)
    home_ids = jnp.arange(experts * direct, dtype=jnp.int32)
    pool_ids = jnp.arange(groups * pooled, dtype=jnp.int32)
    home_pick = (home_ids[:, None] == home_cell[None, :]).astype(jnp.bfloat16)
    pool_pick = (pool_ids[:, None] == pool_cell[None, :]).astype(jnp.bfloat16)
    side = jnp.sum(
        jnp.where(pool_ids[:, None] == pool_cell[None, :], (served % 2)[None, :], 0), axis=1
    )
    side_out = jnp.broadcast_to(side.astype(jnp.float32)[:, None], (groups * pooled, 128))
    unserved = jnp.broadcast_to(jnp.max(left.astype(jnp.int32)), (8, 128))
    home_ret, pool_ret, shared_hidden, unserved_all = routed_exchange(
        home_pick.reshape(experts, direct, tok_count),
        pool_pick.reshape(groups, pooled, tok_count),
        side_out.reshape(groups, pooled, 128),
        unserved,
        token_scale[:, None],
        tokens,
        w_gate,
        w_up,
        w_down,
        shared_gate.T,
        shared_up.T,
    )

    def combined():
        home_back = (home_cell[:, None] == home_ids[None, :]).astype(jnp.bfloat16)
        pool_back = (pool_cell[:, None] == pool_ids[None, :]).astype(jnp.bfloat16)
        pick = jnp.concatenate([home_back, pool_back, shared_hidden], axis=1)
        source = jnp.concatenate(
            [home_ret.reshape(-1, model_width), pool_ret.reshape(-1, model_width), shared_down],
            axis=0,
        )
        return jnp.dot(pick, source, preferred_element_type=jnp.float32)

    def all_served():
        return combined().astype(jnp.bfloat16)

    def some_left():
        rows = (tokens.astype(jnp.float32) * token_scale[:, None]).astype(jnp.bfloat16)
        lanes = home_count + 2 * spill_count
        to_right = host_expert == (expert_id + 1) % experts
        lane_index = jnp.where(
            is_spill,
            home_count + spill_level + jnp.where(to_right, 0, spill_count),
            token_slot,
        )
        cell_index = served * lanes + lane_index
        source_row = jnp.zeros((experts * lanes,), jnp.int32).at[cell_index].set(positions)
        outgoing = rows[source_row].reshape(experts, lanes, model_width)
        incoming = lax.all_to_all(outgoing, "expert", split_axis=0, concat_axis=0, tiled=True)
        answers = lax.all_to_all(
            expert_ffn(incoming, w_gate, w_up, w_down),
            "expert",
            split_axis=0,
            concat_axis=0,
            tiled=True,
        )
        rest = answers.reshape(-1, model_width)[cell_index].astype(jnp.float32)
        return (combined() + jnp.where(left[:, None], rest, 0.0)).astype(jnp.bfloat16)

    return lax.cond(unserved_all[0, 0] > 0, some_left, all_served)


def solution(mesh):
    return jax.shard_map(
        body,
        mesh=mesh,
        in_specs=(
            P(("dp", "expert"), None),
            P(("dp", "expert")),
            P(("dp", "expert")),
            P(("dp", "expert")),
            P(("dp", "expert")),
            P(),
            P("expert", None, None),
            P("expert", None, None),
            P("expert", None, None),
            P(),
            P(),
            P(),
        ),
        out_specs=P(("dp", "expert"), None),
        check_vma=False,
    )
```

```python
import functools

import jax
import jax.numpy as jnp
from jax import lax
from jax.experimental import pallas as pl
from jax.experimental.pallas import tpu as pltpu
from jax.sharding import PartitionSpec as P

MESH = pl.DeviceIdType.MESH


def expert_ffn(inputs, w_gate, w_up, w_down):
    flat_rows = inputs.reshape(-1, inputs.shape[-1])
    gate_out = jnp.dot(flat_rows, w_gate, preferred_element_type=jnp.float32)
    up_out = jnp.dot(flat_rows, w_up, preferred_element_type=jnp.float32)
    hidden = (jax.nn.silu(gate_out) * up_out).astype(jnp.bfloat16)
    result = jnp.dot(hidden, w_down, preferred_element_type=jnp.float32).astype(jnp.bfloat16)
    return result.reshape(inputs.shape)


def flip(index, step, count):
    out, bit = 0, 1
    while bit < count:
        out = out + bit * lax.rem(index // bit + step // bit, 2)
        bit *= 2
    return out


def moe_kernel(
    dps,
    experts,
    groups,
    home_pick,
    pool_pick,
    side_out,
    need_ref,
    scale_ref,
    tok_ref,
    wg_hbm,
    wu_hbm,
    wd_hbm,
    sg_ref,
    su_ref,
    home_ret,
    pool_ret,
    shared_ref,
    need_max,
    need_all,
    routed_in,
    home_out,
    pool_out,
    home_in,
    home_res,
    pool_in,
    pool_res,
    pool_part,
    pool_comb,
    side_in,
    wg,
    wu,
    wd,
    w_sem,
    own_sem,
    ns_sem,
    nr_sem,
    hs_sem,
    hr_sem,
    rs_sem,
    rr_sem,
    zs_sem,
    zr_sem,
    ms_sem,
    mr_sem,
    xs_sem,
    xr_sem,
    ps_sem,
    pr_sem,
    cs_sem,
    cr_sem,
):
    my_dp = lax.axis_index("dp")
    e = lax.axis_index("expert")
    g = e // 2
    p = e - 2 * g
    partner = e + 1 - 2 * p
    total = dps * experts
    me = my_dp * experts + e

    barrier = pltpu.get_barrier_semaphore()

    @pl.loop(1, total)
    def _(k):
        there = lax.rem(me + k, total)
        pl.semaphore_signal(
            barrier,
            inc=1,
            device_id={"dp": there // experts, "expert": lax.rem(there, experts)},
            device_id_type=MESH,
        )

    weights = [
        pltpu.make_async_copy(a, b, w_sem.at[i])
        for i, (a, b) in enumerate(((wg_hbm, wg), (wu_hbm, wu), (wd_hbm, wd)))
    ]
    own = [
        pltpu.make_async_copy(home_out.at[e], home_in.at[e], own_sem.at[0]),
        pltpu.make_async_copy(pool_out.at[g], pool_in.at[0, g], own_sem.at[1]),
        pltpu.make_async_copy(side_out.at[g], side_in.at[g], own_sem.at[2]),
        pltpu.make_async_copy(need_ref, need_all.at[me], own_sem.at[3]),
    ]

    def remote(src, dst, send, recv, to):
        return pltpu.make_async_remote_copy(
            src_ref=src,
            dst_ref=dst,
            send_sem=send,
            recv_sem=recv,
            device_id={"expert": to},
            device_id_type=MESH,
        )

    def n_copy(k):
        there = lax.rem(me + k, total)
        return pltpu.make_async_remote_copy(
            src_ref=need_ref,
            dst_ref=need_all.at[me],
            send_sem=ns_sem.at[k],
            recv_sem=nr_sem.at[k],
            device_id={"dp": there // experts, "expert": lax.rem(there, experts)},
            device_id_type=MESH,
        )

    def z_copy(k):
        to = flip(g, k, groups)
        return remote(pool_out.at[to], pool_in.at[0, g], zs_sem.at[k], zr_sem.at[k], 2 * to + p)

    def m_copy(k):
        to = flip(g, k, groups)
        return remote(side_out.at[to], side_in.at[g], ms_sem.at[k], mr_sem.at[k], 2 * to + p)

    def h_copy(k):
        to = flip(e, k, experts)
        return remote(home_out.at[to], home_in.at[e], hs_sem.at[k], hr_sem.at[k], to)

    def x_copy(k):
        origin = flip(g, k, groups)
        return remote(
            pool_in.at[0, origin],
            pool_in.at[1, flip(g, k, groups)],
            xs_sem.at[k],
            xr_sem.at[k],
            partner,
        )

    def p_copy(k):
        origin = flip(g, k, groups)
        return remote(
            pool_res.at[origin], pool_part.at[origin], ps_sem.at[k], pr_sem.at[k], partner
        )

    def c_copy(k):
        origin = flip(g, k, groups)
        return remote(
            pool_comb.at[origin], pool_ret.at[g], cs_sem.at[k], cr_sem.at[k], 2 * origin + p
        )

    def r_copy(k):
        origin = flip(e, k, experts)
        return remote(home_res.at[origin], home_ret.at[e], rs_sem.at[k], rr_sem.at[k], origin)

    def rows_of(pick):
        return jnp.dot(pick, routed_in[...], preferred_element_type=jnp.float32).astype(jnp.bfloat16)

    routed_in[...] = (tok_ref[...].astype(jnp.float32) * scale_ref[...]).astype(jnp.bfloat16)

    pl.semaphore_wait(barrier, total - 1)

    @pl.loop(1, groups + 1)
    def _(i):
        k = groups - i
        to = flip(g, k, groups)
        pool_out[to] = rows_of(pool_pick[to])

        @pl.when(i > 1)
        def _():
            z_copy(k + 1).start()
            m_copy(k + 1).start()

    @pl.loop(1, experts + 1)
    def _(i):
        k = experts - i
        to = flip(e, k, experts)
        home_out[to] = rows_of(home_pick[to])

        @pl.when(i > 1)
        def _():
            h_copy(k + 1).start()

    for copy in own:
        copy.start()
    for copy in weights:
        copy.start()

    @pl.loop(1, total)
    def _(k):
        n_copy(k).start()

    for copy in own:
        copy.wait()
    x_copy(0).start()

    tok = tok_ref[...]
    last = (((1,), (1,)), ((), ()))
    shared_gate = lax.dot_general(tok, sg_ref[...], last, preferred_element_type=jnp.float32)
    shared_up = lax.dot_general(tok, su_ref[...], last, preferred_element_type=jnp.float32)
    shared_ref[...] = (jax.nn.silu(shared_gate) * shared_up).astype(jnp.bfloat16)

    for copy in weights:
        copy.wait()

    def ffn(x):
        gate_out = jnp.dot(x, wg[...], preferred_element_type=jnp.float32)
        up_out = jnp.dot(x, wu[...], preferred_element_type=jnp.float32)
        hidden = (jax.nn.silu(gate_out) * up_out).astype(jnp.bfloat16)
        return jnp.dot(hidden, wd[...], preferred_element_type=jnp.float32).astype(jnp.bfloat16)

    home_res[e] = ffn(home_in[e])
    own_ret = pltpu.make_async_copy(home_res.at[e], home_ret.at[e], own_sem.at[0])
    own_ret.start()

    @pl.loop(1, groups)
    def _(i):
        k = groups - i
        z_copy(k).wait_recv()
        x_copy(k).start()

    def home_block(i):
        k = experts - i
        origin = flip(e, k, experts)
        h_copy(k).wait_recv()
        home_res[origin] = ffn(home_in[origin])
        r_copy(k).start()

    @pl.loop(1, groups + 1)
    def _(i):
        k = groups - i
        origin = flip(g, k, groups)
        x_copy(k).wait_recv()
        pool_res[origin] = ffn(pool_in[1, origin])
        p_copy(k).start()

    @pl.loop(1, groups + 1)
    def _(i):
        k = groups - i
        origin = flip(g, k, groups)
        mine = ffn(pool_in[0, origin])
        p_copy(k).wait_recv()

        @pl.when(k > 0)
        def _():
            m_copy(k).wait_recv()

        here = jnp.abs(side_in[origin][:, :1] - p.astype(jnp.float32)) < 0.5
        pool_comb[origin] = jnp.where(here, mine, pool_part[origin])

        @pl.when(k > 0)
        def _():
            c_copy(k).start()

    own_back = pltpu.make_async_copy(pool_comb.at[g], pool_ret.at[g], own_sem.at[1])
    own_back.start()

    pl.loop(1, experts)(home_block)

    @pl.loop(0, groups)
    def _(k):
        x_copy(k).wait_send()
        p_copy(k).wait_send()

    @pl.loop(1, groups)
    def _(k):
        z_copy(k).wait_send()
        m_copy(k).wait_send()
        c_copy(k).wait()

    @pl.loop(1, total)
    def _(k):
        n_copy(k).wait()

    @pl.loop(1, experts)
    def _(k):
        h_copy(k).wait_send()
        r_copy(k).wait()

    own_ret.wait()
    own_back.wait()
    need_max[...] = jnp.max(need_all[...], axis=0)


def routed_exchange(
    home_pick, pool_pick, side_out, need, scale, tokens, w_gate, w_up, w_down, shared_gate, shared_up
):
    dps, experts = lax.axis_size("dp"), lax.axis_size("expert")
    groups = pool_pick.shape[0]
    width = tokens.shape[1]
    home_shape, pool_shape = home_pick.shape[:2] + (width,), pool_pick.shape[:2] + (width,)
    bf16 = jnp.bfloat16
    vmem = pl.BlockSpec(memory_space=pltpu.VMEM)
    anywhere = pl.BlockSpec(memory_space=pl.ANY)
    dma = pltpu.SemaphoreType.DMA
    return pl.pallas_call(
        functools.partial(moe_kernel, dps, experts, groups),
        out_shape=(
            jax.ShapeDtypeStruct(home_shape, bf16),
            jax.ShapeDtypeStruct(pool_shape, bf16),
            jax.ShapeDtypeStruct((tokens.shape[0], shared_gate.shape[0]), bf16),
            jax.ShapeDtypeStruct(need.shape, need.dtype),
        ),
        in_specs=[vmem] * 6 + [anywhere] * 3 + [vmem] * 2,
        out_specs=(vmem,) * 4,
        scratch_shapes=[
            pltpu.VMEM((dps * experts,) + need.shape, need.dtype),
            pltpu.VMEM(tokens.shape, bf16),
            pltpu.VMEM(home_shape, bf16),
            pltpu.VMEM(pool_shape, bf16),
            pltpu.VMEM(home_shape, bf16),
            pltpu.VMEM(home_shape, bf16),
            pltpu.VMEM((2,) + pool_shape, bf16),
            pltpu.VMEM(pool_shape, bf16),
            pltpu.VMEM(pool_shape, bf16),
            pltpu.VMEM(pool_shape, bf16),
            pltpu.VMEM(side_out.shape, jnp.float32),
            pltpu.VMEM(w_gate.shape, bf16),
            pltpu.VMEM(w_up.shape, bf16),
            pltpu.VMEM(w_down.shape, bf16),
            dma((3,)),
            dma((4,)),
        ]
        + [dma((dps * experts,))] * 2
        + [dma((experts,))] * 4
        + [dma((groups,))] * 10,
        compiler_params=pltpu.CompilerParams(
            collective_id=0, has_side_effects=True, vmem_limit_bytes=60 * 1024 * 1024
        ),
        name="moe",
    )(home_pick, pool_pick, side_out, need, scale, tokens, w_gate, w_up, w_down, shared_gate, shared_up)


def body(
    tokens,
    router_logit,
    expert_id,
    token_slot,
    keep,
    overflow_host,
    expert_gate,
    expert_up,
    expert_down,
    shared_gate,
    shared_up,
    shared_down,
):
    experts = lax.axis_size("expert")
    dps = lax.axis_size("dp")
    groups = experts // 2
    my_e = lax.axis_index("expert")
    tok_count, model_width = tokens.shape
    slot_count = 2 * tok_count // experts
    home_count = slot_count // 2
    spill_count = slot_count - home_count
    w_gate, w_up, w_down = expert_gate[0], expert_up[0], expert_down[0]
    token_scale = jax.nn.sigmoid(router_logit) * keep.astype(jnp.float32)
    positions = jnp.arange(tok_count, dtype=jnp.int32)
    is_spill = token_slot >= home_count
    spill_level = jnp.maximum(token_slot - home_count, 0)
    table_index = expert_id * spill_count + spill_level
    table_ids = jnp.arange(experts * spill_count, dtype=jnp.int32)
    host_expert = jnp.sum(
        jnp.where(table_index[:, None] == table_ids[None, :], overflow_host.reshape(1, -1), 0),
        axis=1,
    )
    served = jnp.where(is_spill, host_expert, expert_id)
    kept = keep != 0
    before = positions[None, :] < positions[:, None]

    def rank_of(member, label):
        same = (label[:, None] == label[None, :]) & member[None, :] & before
        return jnp.sum(same.astype(jnp.int32), axis=1)

    direct = max(1, 3 * home_count // 4)
    pooled = home_count
    direct_rank = rank_of(kept, served)
    over = kept & (direct_rank >= direct)
    pool_rank = rank_of(over, served // 2)
    left = over & (pool_rank >= pooled)
    home_cell = jnp.where(kept & ~over, served * direct + direct_rank, -1)
    pool_cell = jnp.where(over & ~left, (served // 2) * pooled + pool_rank, -1)
    home_ids = jnp.arange(experts * direct, dtype=jnp.int32)
    pool_ids = jnp.arange(groups * pooled, dtype=jnp.int32)
    home_pick = (home_ids[:, None] == home_cell[None, :]).astype(jnp.bfloat16)
    pool_pick = (pool_ids[:, None] == pool_cell[None, :]).astype(jnp.bfloat16)
    side = jnp.sum(
        jnp.where(pool_ids[:, None] == pool_cell[None, :], (served % 2)[None, :], 0), axis=1
    )
    side_out = jnp.broadcast_to(side.astype(jnp.float32)[:, None], (groups * pooled, 128))
    unserved = jnp.broadcast_to(jnp.max(left.astype(jnp.int32)), (8, 128))
    home_ret, pool_ret, shared_hidden, unserved_all = routed_exchange(
        home_pick.reshape(experts, direct, tok_count),
        pool_pick.reshape(groups, pooled, tok_count),
        side_out.reshape(groups, pooled, 128),
        unserved,
        token_scale[:, None],
        tokens,
        w_gate,
        w_up,
        w_down,
        shared_gate.T,
        shared_up.T,
    )

    def combined():
        home_back = (home_cell[:, None] == home_ids[None, :]).astype(jnp.bfloat16)
        pool_back = (pool_cell[:, None] == pool_ids[None, :]).astype(jnp.bfloat16)
        pick = jnp.concatenate([home_back, pool_back, shared_hidden], axis=1)
        source = jnp.concatenate(
            [home_ret.reshape(-1, model_width), pool_ret.reshape(-1, model_width), shared_down],
            axis=0,
        )
        return jnp.dot(pick, source, preferred_element_type=jnp.float32)

    def all_served():
        return combined().astype(jnp.bfloat16)

    def some_left():
        rows = (tokens.astype(jnp.float32) * token_scale[:, None]).astype(jnp.bfloat16)
        lanes = home_count + 2 * spill_count
        to_right = host_expert == (expert_id + 1) % experts
        lane_index = jnp.where(
            is_spill,
            home_count + spill_level + jnp.where(to_right, 0, spill_count),
            token_slot,
        )
        cell_index = served * lanes + lane_index
        source_row = jnp.zeros((experts * lanes,), jnp.int32).at[cell_index].set(positions)
        outgoing = rows[source_row].reshape(experts, lanes, model_width)
        incoming = lax.all_to_all(outgoing, "expert", split_axis=0, concat_axis=0, tiled=True)
        answers = lax.all_to_all(
            expert_ffn(incoming, w_gate, w_up, w_down),
            "expert",
            split_axis=0,
            concat_axis=0,
            tiled=True,
        )
        rest = answers.reshape(-1, model_width)[cell_index].astype(jnp.float32)
        return (combined() + jnp.where(left[:, None], rest, 0.0)).astype(jnp.bfloat16)

    return lax.cond(unserved_all[0, 0] > 0, some_left, all_served)


def solution(mesh):
    return jax.shard_map(
        body,
        mesh=mesh,
        in_specs=(
            P(("dp", "expert"), None),
            P(("dp", "expert")),
            P(("dp", "expert")),
            P(("dp", "expert")),
            P(("dp", "expert")),
            P(),
            P("expert", None, None),
            P("expert", None, None),
            P("expert", None, None),
            P(),
            P(),
            P(),
        ),
        out_specs=P(("dp", "expert"), None),
        check_vma=False,
    )
```
